128 devices in a mesh: edp: 2 (over y_hi), ep: 64 (over y_lo, z, x, core).
Axes of the slice: x: 4, y: 4 (y_hi: 2, y_lo: 2; y = y_hi * 2 + y_lo), z: 4, core: 2. Of those that a mesh axis runs over, the one named last changes fastest.
Arguments:
- tokens: bfloat16 [16384, 2048], P(('edp', 'ep')), may hold values from -6 to 6
- routes: int32 [16384, 8], P(('edp', 'ep')), may hold values from 0 to 63, all different within a row; in each aligned block of 128 rows (0 to 127, 128 to 255, ...) at most 24 rows name the same one
- gate_weights: float32 [16384, 8], P(('edp', 'ep')), may hold values from 0.05 to 0.5
- w_gate: bfloat16 [64, 2048, 768], P('ep'), may hold values from -0.125 to 0.125
- w_up: bfloat16 [64, 2048, 768], P('ep'), may hold values from -0.125 to 0.125
- w_down: bfloat16 [64, 768, 2048], P('ep'), may hold values from -0.21875 to 0.21875
- saved_inputs: bfloat16 [64, 512, 2048], P('ep', 'edp'), may hold values from -6 to 6
- saved_cotangent: bfloat16 [64, 512, 2048], P('ep', 'edp'), may hold values from -0.59765625 to 0.59765625
Outputs:
- mixed: bfloat16 [16384, 2048], P(('edp', 'ep'))
- grad_gate: float32 [64, 2048, 768], P('ep', 'edp')
- grad_up: float32 [64, 2048, 768], P('ep', 'edp')
- grad_down: float32 [64, 768, 2048], P('ep', 'edp')
The draws below stay inside these ranges and needn't reach their ends.
Inputs may be any that keep to these rules, and one draw needn't show every extreme that they name: `routes`: each token names 8 different experts. In each aligned block of 128 tokens (the tokens of one device) no expert is named more than 24 times, a bound that some block reaches in every draw.
All inputs are finite; a program needn't handle non-finite values.
Results may differ from the reference program's by a relative error of at most 0.006.
Values may be sent and summed in bfloat16 or wider, within the bound.
No kernel may reach another device: no remote copies, remote signals or barrier semaphores. Data moves between devices by JAX's collectives and lax.ppermute only.
A program may use at most 128 MiB of HBM per device.

```python
import math
import jax
import jax.numpy as jnp
import numpy as np
from jax import lax

D = 2048
FF = 768
TOP = 8
TOK_DEV = 128
ROWS_BWD = 256
EXPERTS = 64
CAP = 24
TOKENS = 16384
BWD_ROWS = 512
N_EDP = 2


def levels(rng, dims, split, smallest, largest):
    gain, own = 1.0, jax.random.fold_in(rng, 6)
    for axis_at, blocks in split:
        steps = jnp.exp(jax.random.uniform(jax.random.fold_in(own, axis_at), (blocks,), jnp.float32, smallest / len(split), largest / len(split)))
        gain = gain * jnp.repeat(steps, dims[axis_at] // blocks).reshape([-1 if axis == axis_at else 1 for axis in range(len(dims))])
    return gain


def routed_block(stream_key, own, number, rows, number_of, top, reach, lean):
    order = jax.random.permutation(stream_key, number_of)
    packed, ordinary = portions_of(number_of, rows * top, reach, lean, True), portions_of(number_of, rows * top, reach, lean, False)
    places = jnp.arange(number_of)

    def named(tallies, offset_by):
        used = int((tallies > 0).sum())
        fixed = max(1, used // 4)
        shifted = fixed + (places - fixed + offset_by * (used - fixed)) % max(1, number_of - fixed)
        return jnp.zeros((number_of,), jnp.int32).at[order[jnp.where(places < fixed, places, shifted)]].set(jnp.asarray(tallies, jnp.int32))

    tallies = jnp.where(number % 4 == 0, named(packed, number // 4), named(ordinary, number - number // 4 - 1))
    mixed = jax.random.permutation(jax.random.fold_in(own, 3), number_of)
    source_of, receiver = mixed[0:number_of // 2 * 2:2], mixed[1:number_of // 2 * 2:2]
    margin = jnp.minimum(tallies[source_of] - 1, reach - tallies[receiver]) // 2
    margin = jnp.where((source_of == order[0]) | (receiver == order[0]) | (tallies[receiver] == 0), 0, jnp.maximum(margin, 0))
    shifted = jax.random.randint(jax.random.fold_in(own, 4), (number_of // 2,), 0, 1 << 20) % (margin + 1)
    tallies = tallies.at[source_of].add(-shifted).at[receiver].add(shifted)
    items = jnp.searchsorted(jnp.cumsum(tallies), jnp.arange(rows * top), side="right").astype(jnp.int32)
    listing = items.reshape(top, rows).T
    listing = listing[jax.random.permutation(jax.random.fold_in(own, 1), rows)]
    offset_by = jax.random.randint(jax.random.fold_in(own, 2), (rows, 1), 0, top)
    return jnp.take_along_axis(listing, (jnp.arange(top)[None, :] + offset_by) % top, axis=1)


def portions_of(amount, total, limit, slope, full):
    weights = [(1 << 20) // math.isqrt(rank ** slope) + 1 for rank in range(1, amount + 1)]
    largest = limit if full else min(limit, max(-(-total // amount), total * weights[0] // sum(weights)))
    least = 1 if total - largest >= amount - 1 else 0
    holding, surplus = [largest] + [least] * (amount - 1), total - largest - least * (amount - 1)
    while surplus > 0:
        movable = [i for i in range(1, amount) if holding[i] < largest] or [i for i in range(1, amount) if holding[i] < limit]
        mass, budget = sum([weights[i] for i in movable]), surplus
        for i in movable:
            addition = min(limit - holding[i], max(1, budget * weights[i] // mass), surplus)
            holding[i] = holding[i] + addition
            surplus = surplus - addition
    return np.array(holding)


def noise(own_key, extent, scale, most, shards=(), kind=jnp.bfloat16):
    drawn = jax.random.normal(own_key, extent, jnp.float32) * scale
    if len(shards) > 0:
        drawn = levels(own_key, extent, shards, -0.22, 0.18) * drawn
    return jnp.clip(drawn, min=-most, max=most).astype(kind)


def setup_inputs(seed: int = 0) -> dict:
    streams_of = jax.random.split(jax.random.key(seed), 9)
    tokens = noise(streams_of[0], (TOKENS, D), 1.0, 6.0, ((0, 128),))
    routes_keys = jax.random.split(jax.random.fold_in(streams_of[1], 1), TOKENS // TOK_DEV)
    routes_turns = jax.random.permutation(jax.random.fold_in(streams_of[1], 3), TOKENS // TOK_DEV)
    routes = jax.vmap(lambda own, number: routed_block(jax.random.fold_in(streams_of[1], 2), own, number, TOK_DEV, EXPERTS, TOP, CAP, 2))(routes_keys, routes_turns).reshape((TOKENS, TOP))
    gate_weights = jnp.clip(jnp.exp(math.log(0.5) - 2.3025851 * jax.random.uniform(streams_of[2], (TOKENS, TOP), jnp.float32) ** levels(streams_of[2], (TOKENS, TOP), ((0, 128),), -0.2, 0.2)), 0.05, 0.5)
    w_gate = noise(streams_of[3], (EXPERTS, D, FF), D ** -0.5, 0.125, ((0, 64),))
    w_up = noise(streams_of[4], (EXPERTS, D, FF), D ** -0.5, 0.125, ((0, 64),))
    w_down = noise(streams_of[5], (EXPERTS, FF, D), FF ** -0.5, 0.21875, ((0, 64),))
    saved_inputs = noise(streams_of[6], (EXPERTS, BWD_ROWS, D), 1.0, 6.0, ((0, 64), (1, 2)))
    saved_cotangent = noise(streams_of[7], (EXPERTS, BWD_ROWS, D), 0.1, 0.59765625, ((0, 64), (1, 2)))
    return {"tokens": tokens, "routes": routes, "gate_weights": gate_weights, "w_gate": w_gate, "w_up": w_up, "w_down": w_down, "saved_inputs": saved_inputs, "saved_cotangent": saved_cotangent}


def expert_mlp(row_data, w_gate, w_up, w_down):
    gate_pre = jnp.dot(row_data, w_gate, preferred_element_type=jnp.float32)
    up_pre = jnp.dot(row_data, w_up, preferred_element_type=jnp.float32)
    hidden = (jax.nn.silu(gate_pre) * up_pre).astype(jnp.bfloat16)
    return jnp.dot(hidden, w_down, preferred_element_type=jnp.float32).astype(jnp.bfloat16)


def expert_grads(inputs, cotangent, w_gate, w_up, w_down):
    gate_pre = jnp.dot(inputs, w_gate, preferred_element_type=jnp.float32)
    up_pre = jnp.dot(inputs, w_up, preferred_element_type=jnp.float32)
    activated = jax.nn.silu(gate_pre)
    hidden = (activated * up_pre).astype(jnp.bfloat16)
    d_hidden = jnp.dot(cotangent, w_down.T, preferred_element_type=jnp.float32)
    sigmoid_gate = jax.nn.sigmoid(gate_pre)
    d_gate = (d_hidden * up_pre * sigmoid_gate * (1.0 + gate_pre * (1.0 - sigmoid_gate))).astype(jnp.bfloat16)
    d_up = (d_hidden * activated).astype(jnp.bfloat16)
    return hidden, d_gate, d_up


def rounded(value):
    return lax.optimization_barrier(value.astype(jnp.bfloat16)).astype(jnp.float32)


def reference(tokens, routes, gate_weights, w_gate, w_up, w_down, saved_inputs, saved_cotangent):
    blocks = TOKENS // TOK_DEV
    route_blocks = routes.reshape(blocks, TOK_DEV * TOP)
    one_hot = (route_blocks[:, :, None] == jnp.arange(EXPERTS, dtype=jnp.int32)[None, None, :]).astype(jnp.int32)
    running = jnp.cumsum(one_hot, axis=1) - 1
    slot_index = jnp.sum(running * one_hot, axis=2)
    position = jnp.arange(blocks, dtype=jnp.int32)[:, None] * CAP + slot_index
    token_id = (jnp.arange(TOKENS * TOP, dtype=jnp.int32) // TOP).astype(jnp.int32)
    row_count = blocks * CAP
    row_table = jnp.full((EXPERTS, row_count), TOKENS, jnp.int32)
    row_table = row_table.at[route_blocks.reshape(-1), position.reshape(-1)].set(token_id)
    weight_table = jnp.zeros((EXPERTS, row_count), jnp.float32)
    weight_table = weight_table.at[route_blocks.reshape(-1), position.reshape(-1)].set(gate_weights.reshape(-1))
    padded = jnp.concatenate([tokens, jnp.zeros((1, D), tokens.dtype)], axis=0)

    def one_expert(accum_rows, expert_data):
        row_ids, weights, gate_mat, up_mat, down_mat = expert_data
        output = expert_mlp(padded[row_ids], gate_mat, up_mat, down_mat)
        accum_rows = accum_rows.at[row_ids].add(weights[:, None] * output.astype(jnp.float32))
        return accum_rows, None

    summed, unused = lax.scan(one_expert, jnp.zeros((TOKENS + 1, D), jnp.float32),
                              (row_table, weight_table, w_gate, w_up, w_down))
    mixed = summed[:TOKENS].astype(jnp.bfloat16)

    def expert_backward(expert_data):
        inputs_all, cotangent_all, gate_mat, up_mat, down_mat = expert_data
        grad_g = jnp.zeros((D, FF), jnp.float32)
        grad_u = jnp.zeros((D, FF), jnp.float32)
        grad_d = jnp.zeros((FF, D), jnp.float32)
        for replica in range(N_EDP):
            inputs = inputs_all[replica * ROWS_BWD:(replica + 1) * ROWS_BWD]
            cotangent = cotangent_all[replica * ROWS_BWD:(replica + 1) * ROWS_BWD]
            hidden, d_gate, d_up = expert_grads(inputs, cotangent, gate_mat, up_mat, down_mat)
            grad_g = grad_g + rounded(jnp.dot(inputs.T, d_gate, preferred_element_type=jnp.float32))
            grad_u = grad_u + rounded(jnp.dot(inputs.T, d_up, preferred_element_type=jnp.float32))
            grad_d = grad_d + rounded(jnp.dot(hidden.T, cotangent, preferred_element_type=jnp.float32))
        return grad_g, grad_u, grad_d

    grad_gate, grad_up, grad_down = lax.map(expert_backward, (saved_inputs, saved_cotangent, w_gate, w_up, w_down))
    return mixed, grad_gate, grad_up, grad_down
```

```python
import jax
import jax.numpy as jnp
from jax import lax
from jax.sharding import PartitionSpec as P


def expert_mlp(row_data, w_gate, w_up, w_down):
    gate_pre = jnp.dot(row_data, w_gate, preferred_element_type=jnp.float32)
    up_pre = jnp.dot(row_data, w_up, preferred_element_type=jnp.float32)
    hidden = (jax.nn.silu(gate_pre) * up_pre).astype(jnp.bfloat16)
    return jnp.dot(hidden, w_down, preferred_element_type=jnp.float32).astype(jnp.bfloat16)


def expert_grads(inputs, cotangent, w_gate, w_up, w_down):
    gate_pre = jnp.dot(inputs, w_gate, preferred_element_type=jnp.float32)
    up_pre = jnp.dot(inputs, w_up, preferred_element_type=jnp.float32)
    activated = jax.nn.silu(gate_pre)
    hidden = (activated * up_pre).astype(jnp.bfloat16)
    d_hidden = jnp.einsum("rd,fd->rf", cotangent, w_down, preferred_element_type=jnp.float32)
    sigmoid_gate = jax.nn.sigmoid(gate_pre)
    d_gate = (d_hidden * up_pre * sigmoid_gate * (1.0 + gate_pre * (1.0 - sigmoid_gate))).astype(
        jnp.bfloat16
    )
    d_up = (d_hidden * activated).astype(jnp.bfloat16)
    return (hidden, d_gate, d_up)


def rounded(value):
    return lax.optimization_barrier(value.astype(jnp.bfloat16)).astype(jnp.float32)


def slot_table(routes, experts):
    named = jnp.any(
        routes[:, :, None] == jnp.arange(experts, dtype=jnp.int32)[None, None, :], axis=1
    )
    rows = routes.shape[0]
    earlier = (
        lax.broadcasted_iota(jnp.int32, (rows, rows), 1)
        < lax.broadcasted_iota(jnp.int32, (rows, rows), 0)
    ).astype(jnp.bfloat16)
    before = jnp.dot(earlier, named.astype(jnp.bfloat16), preferred_element_type=jnp.float32)
    return jnp.where(named, before.astype(jnp.int32), -1)


def select_rows(slots, capacity, tokens):
    rows, experts = slots.shape
    chosen = slots.T[:, None, :] == jnp.arange(capacity, dtype=jnp.int32)[None, :, None]
    chosen = chosen.astype(jnp.bfloat16).reshape(experts * capacity, rows)
    return jnp.dot(chosen, tokens, preferred_element_type=jnp.float32).astype(jnp.bfloat16)


def combine_rows(slots, routes, gate_weights, capacity, returned):
    rows, experts = slots.shape
    weight = jnp.sum(
        jnp.where(
            routes[:, :, None] == jnp.arange(experts, dtype=jnp.int32)[None, None, :],
            gate_weights[:, :, None],
            0.0,
        ),
        axis=1,
    )
    high = lax.reduce_precision(weight, 8, 7)
    low = weight - high
    both = jnp.concatenate([high, low], axis=0).astype(jnp.bfloat16)
    place = jnp.concatenate([slots, slots], axis=0)
    spread = jnp.where(
        place[:, :, None] == jnp.arange(capacity, dtype=jnp.int32)[None, None, :],
        both[:, :, None],
        jnp.bfloat16(0.0),
    ).reshape(2 * rows, experts * capacity)
    halves = jnp.dot(spread, returned, preferred_element_type=jnp.float32)
    return halves[:rows] + halves[rows:]


def shards(tokens, routes, gate_weights, w_gate, w_up, w_down, saved_inputs, saved_cotangent):
    experts = lax.axis_size("ep")
    tok_rows, width = tokens.shape
    top_count = routes.shape[1]
    capacity = 3 * tok_rows * top_count // (2 * experts)
    gate_mat, up_mat, down_mat = (w_gate[0], w_up[0], w_down[0])
    replicas = lax.axis_size("edp")
    ring = [(r, (r + 1) % replicas) for r in range(replicas)]

    slots = slot_table(routes, experts)
    send_buffer = select_rows(slots, capacity, tokens).reshape(experts, capacity, width)
    received = lax.all_to_all(send_buffer, "ep", split_axis=0, concat_axis=0, tiled=True)
    output = expert_mlp(received.reshape(-1, width), gate_mat, up_mat, down_mat)
    returned = lax.all_to_all(
        output.reshape(received.shape), "ep", split_axis=0, concat_axis=0, tiled=True
    ).reshape(experts * capacity, width)
    combined = combine_rows(slots, routes, gate_weights, capacity, returned).astype(jnp.bfloat16)

    own_index = lax.axis_index("edp")
    half_width = width // replicas
    half_hidden = gate_mat.shape[1] // replicas
    grad_g = jnp.zeros((half_width, gate_mat.shape[1]), jnp.float32)
    grad_u = jnp.zeros((half_width, gate_mat.shape[1]), jnp.float32)
    grad_d = jnp.zeros((half_hidden, width), jnp.float32)
    inputs, cotangent = saved_inputs[0], saved_cotangent[0]
    for replica in range(replicas):
        hidden, d_gate, d_up = expert_grads(inputs, cotangent, gate_mat, up_mat, down_mat)
        in_cols = lax.dynamic_slice_in_dim(inputs, own_index * half_width, half_width, 1)
        hidden_cols = lax.dynamic_slice_in_dim(hidden, own_index * half_hidden, half_hidden, 1)
        grad_g = grad_g + rounded(
            jnp.einsum("rd,rf->df", in_cols, d_gate, preferred_element_type=jnp.float32)
        )
        grad_u = grad_u + rounded(
            jnp.einsum("rd,rf->df", in_cols, d_up, preferred_element_type=jnp.float32)
        )
        grad_d = grad_d + rounded(
            jnp.einsum("rf,rd->fd", hidden_cols, cotangent, preferred_element_type=jnp.float32)
        )
        if replica + 1 < replicas:
            inputs = lax.ppermute(inputs, "edp", ring)
            cotangent = lax.ppermute(cotangent, "edp", ring)
    grad_gate, grad_up, grad_down = (grad_g[None], grad_u[None], grad_d[None])
    return (combined, grad_gate, grad_up, grad_down)


def solution(mesh):
    return jax.shard_map(
        shards,
        mesh=mesh,
        in_specs=(
            P(("edp", "ep"), None),
            P(("edp", "ep"), None),
            P(("edp", "ep"), None),
            P("ep", None, None),
            P("ep", None, None),
            P("ep", None, None),
            P("ep", "edp", None),
            P("ep", "edp", None),
        ),
        out_specs=(
            P(("edp", "ep"), None),
            P("ep", "edp", None),
            P("ep", "edp", None),
            P("ep", "edp", None),
        ),
        check_vma=False,
    )
```

```python
import jax
import jax.numpy as jnp
from jax import lax
from jax.experimental import pallas as pl
from jax.experimental.pallas import tpu as pltpu
from jax.sharding import Mesh, PartitionSpec as P

VMEM_LIMIT = 56 * 2**20


def expert_grads(inputs, cotangent, w_gate, w_up, w_down):
    gate_pre = jnp.dot(inputs, w_gate, preferred_element_type=jnp.float32)
    up_pre = jnp.dot(inputs, w_up, preferred_element_type=jnp.float32)
    activated = jax.nn.silu(gate_pre)
    hidden = (activated * up_pre).astype(jnp.bfloat16)
    d_hidden = jnp.einsum("rd,fd->rf", cotangent, w_down, preferred_element_type=jnp.float32)
    sigmoid_gate = jax.nn.sigmoid(gate_pre)
    d_gate = (d_hidden * up_pre * sigmoid_gate * (1.0 + gate_pre * (1.0 - sigmoid_gate))).astype(
        jnp.bfloat16
    )
    d_up = (d_hidden * activated).astype(jnp.bfloat16)
    return (hidden, d_gate, d_up)


def rounded(value):
    return lax.optimization_barrier(value.astype(jnp.bfloat16)).astype(jnp.float32)


def slot_table(named):
    tokens = named.shape[1]
    earlier = (
        lax.broadcasted_iota(jnp.int32, (tokens, tokens), 0)
        < lax.broadcasted_iota(jnp.int32, (tokens, tokens), 1)
    ).astype(jnp.bfloat16)
    before = jnp.dot(named.astype(jnp.bfloat16), earlier, preferred_element_type=jnp.float32)
    return jnp.where(named, before.astype(jnp.int32), -1)


def named_by(routes, first, experts):
    return routes.T[:, None, :] == first + jnp.arange(experts, dtype=jnp.int32)[None, :, None]


def select_rows(place, tokens, count):
    experts, rows = place.shape
    width = tokens.shape[1]
    step = 256 // count

    def kernel(place_ref, token_ref, out_ref):
        chosen = place_ref[...][:, None, :] == lax.broadcasted_iota(
            jnp.int32, (step, count, rows), 1
        )
        chosen = jnp.where(chosen, 1.0, 0.0).reshape(step * count, rows).astype(jnp.bfloat16)
        out_ref[...] = jnp.dot(
            chosen, token_ref[...], preferred_element_type=jnp.float32
        ).astype(jnp.bfloat16)

    return pl.pallas_call(
        kernel,
        grid=(experts // step,),
        in_specs=[
            pl.BlockSpec((step, rows), lambda i: (i, 0)),
            pl.BlockSpec((rows, width), lambda i: (0, 0)),
        ],
        out_specs=pl.BlockSpec((step * count, width), lambda i: (i, 0)),
        out_shape=jax.ShapeDtypeStruct((experts * count, width), jnp.bfloat16),
        cost_estimate=pl.CostEstimate(
            flops=2 * experts * count * rows * width,
            bytes_accessed=2 * (experts * count + rows) * width,
            transcendentals=0,
        ),
        compiler_params=pltpu.CompilerParams(vmem_limit_bytes=VMEM_LIMIT),
    )(place, tokens)


def expert_mlp(row_data, w_gate, w_up, w_down, out_shape, slot, slots, store, into=None):
    rows, width = row_data.shape
    hidden_size = w_gate.shape[1]
    step = 256
    steps = hidden_size // step

    def kernel(x_ref, gate_ref, up_ref, down_ref, *rest):
        out_ref, sum_ref, stage_ref, sem = rest[-4:]
        x = x_ref[...]
        gate_pre = jnp.dot(x, gate_ref[...], preferred_element_type=jnp.float32)
        up_pre = jnp.dot(x, up_ref[...], preferred_element_type=jnp.float32)
        hidden = (jax.nn.silu(gate_pre) * up_pre).astype(jnp.bfloat16)
        part = jnp.dot(hidden, down_ref[...], preferred_element_type=jnp.float32)
        at = pl.program_id(0)

        @pl.when(at == 0)
        def _():
            sum_ref[...] = part

        @pl.when((at > 0) & (at < steps - 1))
        def _():
            sum_ref[...] += part

        @pl.when(at == steps - 1)
        def _():
            store(stage_ref, sum_ref[...] + part)
            copy = pltpu.make_async_copy(stage_ref, out_ref.at[:, slot : slot + slots, :], sem)
            copy.start()
            copy.wait()

    operands = [row_data, w_gate, w_up, w_down]
    in_specs = [
        pl.BlockSpec((rows, width), lambda j: (0, 0)),
        pl.BlockSpec((width, step), lambda j: (0, j)),
        pl.BlockSpec((width, step), lambda j: (0, j)),
        pl.BlockSpec((step, width), lambda j: (j, 0)),
    ]
    aliases = {}
    if into is not None:
        operands.append(into)
        in_specs.append(pl.BlockSpec(memory_space=pl.ANY))
        aliases = {4: 0}
    return pl.pallas_call(
        kernel,
        grid=(steps,),
        in_specs=in_specs,
        out_specs=pl.BlockSpec(memory_space=pl.ANY),
        out_shape=jax.ShapeDtypeStruct(out_shape, jnp.bfloat16),
        scratch_shapes=[
            pltpu.VMEM((rows, width), jnp.float32),
            pltpu.VMEM((out_shape[0], slots, width), jnp.bfloat16),
            pltpu.SemaphoreType.DMA,
        ],
        input_output_aliases=aliases,
        cost_estimate=pl.CostEstimate(
            flops=6 * rows * width * hidden_size,
            bytes_accessed=2 * (2 * rows + 3 * hidden_size) * width,
            transcendentals=rows * hidden_size,
        ),
        compiler_params=pltpu.CompilerParams(vmem_limit_bytes=VMEM_LIMIT),
    )(*operands)


def weighted_sum(spread, returned):
    terms, rows = spread.shape
    width = returned.shape[1]
    tokens = terms // 2
    step = 512

    def kernel(spread_ref, row_ref, out_ref):
        both = jnp.dot(spread_ref[...], row_ref[...], preferred_element_type=jnp.float32)
        out_ref[...] = (both[:tokens] + both[tokens:]).astype(jnp.bfloat16)

    return pl.pallas_call(
        kernel,
        grid=(width // step,),
        in_specs=[
            pl.BlockSpec((terms, rows), lambda j: (0, 0)),
            pl.BlockSpec((rows, step), lambda j: (0, j)),
        ],
        out_specs=pl.BlockSpec((tokens, step), lambda j: (0, j)),
        out_shape=jax.ShapeDtypeStruct((tokens, width), jnp.bfloat16),
        cost_estimate=pl.CostEstimate(
            flops=2 * terms * rows * width, bytes_accessed=2 * rows * width, transcendentals=0
        ),
        compiler_params=pltpu.CompilerParams(vmem_limit_bytes=VMEM_LIMIT),
    )(spread, returned)


def exchange(value, axes):
    return lax.all_to_all(value, axes, split_axis=0, concat_axis=0, tiled=True)


def layer(tokens, routes, gate_weights, w_gate, w_up, w_down, saved_inputs, saved_cotangent):
    halves, plane = lax.axis_size("half"), lax.axis_size("plane")
    every = ("half", "plane")
    experts = halves * plane
    tok_rows, width = tokens.shape
    top_count = routes.shape[1]
    capacity = 3 * tok_rows * top_count // (2 * experts)
    early = 2 * capacity // 3
    late = capacity - early
    gate_mat, up_mat, down_mat = (w_gate[0], w_up[0], w_down[0])
    replicas = lax.axis_size("edp")
    ring = [(r, (r + 1) % replicas) for r in range(replicas)]
    swap = [(0, 1), (1, 0)]
    half = lax.axis_index("half")

    other_routes = lax.ppermute(routes, "half", swap)
    other_tokens = lax.ppermute(tokens, "half", swap)

    named = named_by(routes, 0, experts)
    slots = slot_table(jnp.any(named, axis=0))
    send1 = select_rows(slots, tokens, early)
    received1 = exchange(send1.reshape(experts, early, width), every)
    is_low = half == 0
    low_routes = jnp.where(is_low, routes, other_routes)
    high_routes = jnp.where(is_low, other_routes, routes)
    low_tokens = jnp.where(is_low, tokens, other_tokens)
    high_tokens = jnp.where(is_low, other_tokens, tokens)
    places = []
    for number, block_routes in enumerate((low_routes, high_routes)):
        place = slot_table(jnp.any(named_by(block_routes, half * plane, plane), axis=0))
        places.append(jnp.where(place >= early, place - early + number * late, -1))
    send2 = select_rows(
        jnp.concatenate(places, axis=1),
        jnp.concatenate([low_tokens, high_tokens], axis=0),
        halves * late,
    )
    received2 = exchange(send2.reshape(plane, halves * late, width), "plane")

    def store1(stage_ref, value):
        stage_ref[...] = value.reshape(experts, early, width).astype(jnp.bfloat16)

    def store2(stage_ref, value):
        value = value.reshape(plane, halves, late, width)
        for number in range(halves):
            stage_ref[number * plane : (number + 1) * plane] = value[:, number].astype(jnp.bfloat16)

    shape = (experts, capacity, width)
    output = expert_mlp(
        received1.reshape(-1, width), gate_mat, up_mat, down_mat,
        shape, 0, early, store1,
    )
    output = expert_mlp(
        received2.reshape(-1, width), gate_mat, up_mat, down_mat,
        shape, early, late, store2, into=output,
    )
    returned = exchange(output, every)

    weight = jnp.sum(jnp.where(named, gate_weights.T[:, None, :], 0.0), axis=0).T
    high = lax.reduce_precision(weight, 8, 7)
    terms = jnp.concatenate([high, weight - high], axis=0).astype(jnp.bfloat16)
    place = jnp.concatenate([slots.T, slots.T], axis=0)
    spread = jnp.where(
        place[:, :, None] == jnp.arange(capacity, dtype=jnp.int32)[None, None, :],
        terms[:, :, None],
        jnp.bfloat16(0.0),
    ).reshape(2 * tok_rows, experts * capacity)
    combined = weighted_sum(spread, returned.reshape(-1, width))

    own_index = lax.axis_index("edp")
    half_width = width // replicas
    half_hidden = gate_mat.shape[1] // replicas
    grad_g = jnp.zeros((half_width, gate_mat.shape[1]), jnp.float32)
    grad_u = jnp.zeros((half_width, gate_mat.shape[1]), jnp.float32)
    grad_d = jnp.zeros((half_hidden, width), jnp.float32)
    inputs, cotangent = saved_inputs[0], saved_cotangent[0]
    for replica in range(replicas):
        hidden, d_gate, d_up = expert_grads(inputs, cotangent, gate_mat, up_mat, down_mat)
        in_cols = lax.dynamic_slice_in_dim(inputs, own_index * half_width, half_width, 1)
        hidden_cols = lax.dynamic_slice_in_dim(hidden, own_index * half_hidden, half_hidden, 1)
        grad_g = grad_g + rounded(
            jnp.einsum("rd,rf->df", in_cols, d_gate, preferred_element_type=jnp.float32)
        )
        grad_u = grad_u + rounded(
            jnp.einsum("rd,rf->df", in_cols, d_up, preferred_element_type=jnp.float32)
        )
        grad_d = grad_d + rounded(
            jnp.einsum("rf,rd->fd", hidden_cols, cotangent, preferred_element_type=jnp.float32)
        )
        if replica + 1 < replicas:
            inputs = lax.ppermute(inputs, "edp", ring)
            cotangent = lax.ppermute(cotangent, "edp", ring)
    grad_gate, grad_up, grad_down = (grad_g[None], grad_u[None], grad_d[None])
    return (combined, grad_gate, grad_up, grad_down)


def solution(mesh):
    replicas, ep = mesh.devices.shape
    split = Mesh(mesh.devices.reshape(replicas, 2, ep // 2), ("edp", "half", "plane"))
    tok, own, rep = P(("edp", "half", "plane"), None), ("half", "plane"), "edp"
    return jax.shard_map(
        layer,
        mesh=split,
        in_specs=(tok, tok, tok, P(own), P(own), P(own), P(own, rep, None), P(own, rep, None)),
        out_specs=(tok, P(own, rep, None), P(own, rep, None), P(own, rep, None)),
        check_vma=False,
    )
```

```python
import jax
import jax.numpy as jnp
from jax import lax
from jax.experimental import pallas as pl
from jax.experimental.pallas import tpu as pltpu
from jax.sharding import Mesh, PartitionSpec as P

VMEM_LIMIT = 56 * 2**20
HALVES, RING, CORES = 2, 4, 2
PLANE = ("z", "x", "core")
NOTE_ROWS = 8


def expert_grads(inputs, cotangent, w_gate, w_up, w_down):
    gate_pre = jnp.dot(inputs, w_gate, preferred_element_type=jnp.float32)
    up_pre = jnp.dot(inputs, w_up, preferred_element_type=jnp.float32)
    activated = jax.nn.silu(gate_pre)
    hidden = (activated * up_pre).astype(jnp.bfloat16)
    d_hidden = jnp.einsum("rd,fd->rf", cotangent, w_down, preferred_element_type=jnp.float32)
    sigmoid_gate = jax.nn.sigmoid(gate_pre)
    d_gate = (d_hidden * up_pre * sigmoid_gate * (1.0 + gate_pre * (1.0 - sigmoid_gate))).astype(
        jnp.bfloat16
    )
    d_up = (d_hidden * activated).astype(jnp.bfloat16)
    return (hidden, d_gate, d_up)


def rounded(value):
    return lax.optimization_barrier(value.astype(jnp.bfloat16)).astype(jnp.float32)


def send(value, dz, dx, flip=0):
    if dz % RING == 0 and dx % RING == 0 and not flip:
        return value
    pairs = []
    for z in range(RING):
        for x in range(RING):
            for core in range(CORES):
                source = (z * RING + x) * CORES + core
                target = ((z + dz) % RING * RING + (x + dx) % RING) * CORES + (core ^ flip)
                pairs.append((source, target))
    return lax.ppermute(value, PLANE, pairs)


def annotated(token_cols, routes, gate_weights):
    cols = token_cols.shape[1]
    high = lax.reduce_precision(gate_weights, 8, 7)
    low = gate_weights - high
    note = jnp.concatenate([routes.T.astype(jnp.float32), high.T, low.T], axis=1)
    note = jnp.pad(note, ((0, 0), (0, cols - note.shape[1]))).astype(jnp.bfloat16)
    return jnp.concatenate([token_cols, note], axis=0)


def select_rows(experts, own, other, capacity):
    rings = len(own)
    count = experts.shape[0]
    rows, cols = own[0].shape
    tokens = rows - NOTE_ROWS
    pair = 2 * capacity

    def kernel(expert_ref, *refs):
        own_refs, other_refs = refs[:rings], refs[rings : 2 * rings]
        out_refs = refs[2 * rings : 2 * rings + count]
        place_ref, weight_ref = refs[2 * rings + count :]
        wide = (2 * tokens, 2 * tokens)
        before_at = lax.broadcasted_iota(jnp.int32, wide, 0)
        at = lax.broadcasted_iota(jnp.int32, wide, 1)
        earlier = (before_at < at) & ((before_at >= tokens) == (at >= tokens))
        earlier = jnp.where(earlier, 1.0, 0.0).astype(jnp.bfloat16)
        second = lax.broadcasted_iota(jnp.int32, (count, 2 * tokens), 1) >= tokens
        slot_at = lax.broadcasted_iota(jnp.int32, (count, pair, 2 * tokens), 1)
        for r in range(rings):
            both = (own_refs[r], other_refs[r])
            notes = [ref[tokens:rows, : 3 * tokens].astype(jnp.float32) for ref in both]
            routes = jnp.concatenate([note[:, :tokens] for note in notes], axis=1)
            weights = jnp.concatenate(
                [note[:, tokens : 2 * tokens] + note[:, 2 * tokens :] for note in notes], axis=1
            )
            named, weight = [], []
            for e in range(count):
                hit = routes == expert_ref[e].astype(jnp.float32)
                named.append(jnp.max(jnp.where(hit, 1.0, 0.0), axis=0, keepdims=True))
                weight.append(jnp.sum(jnp.where(hit, weights, 0.0), axis=0, keepdims=True))
            named = jnp.concatenate(named, axis=0)
            before = jnp.dot(
                named.astype(jnp.bfloat16), earlier, preferred_element_type=jnp.float32
            ).astype(jnp.int32)
            place = jnp.where(named > 0.5, before + jnp.where(second, capacity, 0), -1)
            place_ref[r] = place
            weight_ref[r] = jnp.concatenate(weight, axis=0)
            chosen = jnp.where(place[:, None, :] == slot_at, 1.0, 0.0)
            chosen = chosen.reshape(count * pair, 2 * tokens).astype(jnp.bfloat16)
            data = jnp.concatenate([ref[:tokens, :] for ref in both], axis=0)
            result = jnp.dot(chosen, data, preferred_element_type=jnp.float32).astype(jnp.bfloat16)
            for e in range(count):
                out_refs[e][r * pair : (r + 1) * pair, :] = result[e * pair : (e + 1) * pair]

    table = (rings, count, 2 * tokens)
    results = pl.pallas_call(
        kernel,
        in_specs=[pl.BlockSpec(memory_space=pltpu.SMEM)]
        + [pl.BlockSpec((rows, cols), lambda: (0, 0))] * (2 * rings),
        out_specs=[pl.BlockSpec((rings * pair, cols), lambda: (0, 0))] * count
        + [pl.BlockSpec(table, lambda: (0, 0, 0))] * 2,
        out_shape=[jax.ShapeDtypeStruct((rings * pair, cols), jnp.bfloat16)] * count
        + [jax.ShapeDtypeStruct(table, jnp.int32), jax.ShapeDtypeStruct(table, jnp.float32)],
        cost_estimate=pl.CostEstimate(
            flops=4 * rings * count * pair * tokens * cols,
            bytes_accessed=2 * rings * (2 * rows + count * pair) * cols,
            transcendentals=0,
        ),
        compiler_params=pltpu.CompilerParams(vmem_limit_bytes=VMEM_LIMIT),
    )(experts, *own, *other)
    return results[:count], results[count], results[count + 1]


def combine_rows(pieces, place, weight, capacity):
    count = len(pieces)
    rings, _, both_tokens = place.shape
    tokens = both_tokens // 2
    cols = pieces[0].shape[1]
    pair = 2 * capacity

    def kernel(place_ref, weight_ref, *refs):
        piece_refs, own_refs, other_refs = refs[:count], refs[count : count + rings], refs[count + rings :]
        slot_at = lax.broadcasted_iota(jnp.int32, (count, pair, both_tokens), 1)
        for r in range(rings):
            spread = jnp.where(place_ref[r][:, None, :] == slot_at, weight_ref[r][:, None, :], 0.0)
            spread = spread.reshape(count * pair, both_tokens)
            high = spread.astype(jnp.bfloat16)
            low = (spread - high.astype(jnp.float32)).astype(jnp.bfloat16)
            rows = jnp.concatenate([ref[r * pair : (r + 1) * pair, :] for ref in piece_refs], axis=0)
            sums = lax.dot_general(
                jnp.concatenate([high, low], axis=1),
                rows,
                (((0,), (0,)), ((), ())),
                preferred_element_type=jnp.float32,
            )
            sums = (sums[:both_tokens] + sums[both_tokens:]).astype(jnp.bfloat16)
            own_refs[r][...] = sums[:tokens]
            other_refs[r][...] = sums[tokens:]

    table = (rings, count, both_tokens)
    results = pl.pallas_call(
        kernel,
        in_specs=[pl.BlockSpec(table, lambda: (0, 0, 0))] * 2
        + [pl.BlockSpec((rings * pair, cols), lambda: (0, 0))] * count,
        out_specs=[pl.BlockSpec((tokens, cols), lambda: (0, 0))] * (2 * rings),
        out_shape=[jax.ShapeDtypeStruct((tokens, cols), jnp.bfloat16)] * (2 * rings),
        cost_estimate=pl.CostEstimate(
            flops=8 * rings * count * pair * tokens * cols,
            bytes_accessed=2 * rings * (2 * tokens + count * pair) * cols,
            transcendentals=0,
        ),
        compiler_params=pltpu.CompilerParams(vmem_limit_bytes=VMEM_LIMIT),
    )(place, weight, *pieces)
    return results[:rings], results[rings:]


def expert_mlp(left, right, w_gate, w_up, w_down, pair):
    rings = len(left)
    piece_rows, cols = left[0].shape
    rows, width = rings * piece_rows, 2 * cols
    hidden_size = w_gate.shape[1]
    step = 256
    steps = hidden_size // step

    def kernel(*refs):
        left_refs, right_refs = refs[:rings], refs[rings : 2 * rings]
        gate_ref, up_ref, down_ref = refs[2 * rings : 2 * rings + 3]
        left_outs = refs[2 * rings + 3 : 3 * rings + 3]
        right_outs = refs[3 * rings + 3 : 4 * rings + 3]
        x_ref, sum_ref = refs[4 * rings + 3 :]
        at = pl.program_id(0)

        @pl.when(at == 0)
        def _():
            for x in range(rings):
                for z in range(rings):
                    here = pl.ds((x * rings + z) * pair, pair)
                    x_ref[here, :cols] = left_refs[z][x * pair : (x + 1) * pair, :]
                    x_ref[here, cols:] = right_refs[x][z * pair : (z + 1) * pair, :]

        data = x_ref[...]
        gate_pre = jnp.dot(data, gate_ref[...], preferred_element_type=jnp.float32)
        up_pre = jnp.dot(data, up_ref[...], preferred_element_type=jnp.float32)
        hidden = (jax.nn.silu(gate_pre) * up_pre).astype(jnp.bfloat16)
        part = jnp.dot(hidden, down_ref[...], preferred_element_type=jnp.float32)

        @pl.when(at == 0)
        def _():
            sum_ref[...] = part

        @pl.when((at > 0) & (at < steps - 1))
        def _():
            sum_ref[...] += part

        @pl.when(at == steps - 1)
        def _():
            result = (sum_ref[...] + part).astype(jnp.bfloat16)
            for x in range(rings):
                for z in range(rings):
                    here = result[(x * rings + z) * pair : (x * rings + z + 1) * pair]
                    left_outs[z][x * pair : (x + 1) * pair, :] = here[:, :cols]
                    right_outs[x][z * pair : (z + 1) * pair, :] = here[:, cols:]

    piece = pl.BlockSpec((piece_rows, cols), lambda j: (0, 0))
    results = pl.pallas_call(
        kernel,
        grid=(steps,),
        in_specs=[piece] * (2 * rings)
        + [
            pl.BlockSpec((width, step), lambda j: (0, j)),
            pl.BlockSpec((width, step), lambda j: (0, j)),
            pl.BlockSpec((step, width), lambda j: (j, 0)),
        ],
        out_specs=[piece] * (2 * rings),
        out_shape=[jax.ShapeDtypeStruct((piece_rows, cols), jnp.bfloat16)] * (2 * rings),
        scratch_shapes=[
            pltpu.VMEM((rows, width), jnp.bfloat16),
            pltpu.VMEM((rows, width), jnp.float32),
        ],
        cost_estimate=pl.CostEstimate(
            flops=6 * rows * width * hidden_size,
            bytes_accessed=2 * (2 * rows + 3 * hidden_size) * width,
            transcendentals=rows * hidden_size,
        ),
        compiler_params=pltpu.CompilerParams(vmem_limit_bytes=VMEM_LIMIT),
    )(*left, *right, w_gate, w_up, w_down)
    return results[:rings], results[rings:]


def forward(tokens, routes, gate_weights, gate_mat, up_mat, down_mat):
    tok_rows, width = tokens.shape
    top_count = routes.shape[1]
    experts = HALVES * RING * RING * CORES
    capacity = 3 * tok_rows * top_count // (2 * experts)
    cols = width // 2
    swap = [(0, 1), (1, 0)]
    half, z, x, core = (lax.axis_index(name) for name in ("half", "z", "x", "core"))
    ring = range(RING)

    mine = [annotated(tokens[:, side * cols : (side + 1) * cols], routes, gate_weights) for side in (0, 1)]
    other = [lax.ppermute(part, "half", swap) for part in mine]
    lines = []
    for block in (mine, other):
        lines.append(([send(block[0], 0, r) for r in ring], [send(block[1], r, 0) for r in ring]))
    (own_left, own_right), (other_left, other_right) = lines

    targets = [(r, flip) for flip in range(CORES) for r in ring]
    first = half * (RING * RING * CORES)
    left_ids = jnp.stack(
        [first + ((z + r) % RING * RING + x) * CORES + (core ^ flip) for r, flip in targets]
    )
    right_ids = jnp.stack(
        [first + (z * RING + (x + r) % RING) * CORES + (core ^ flip) for r, flip in targets]
    )
    left_rows, left_place, left_weight = select_rows(left_ids, own_left, other_left, capacity)
    right_rows, right_place, right_weight = select_rows(right_ids, own_right, other_right, capacity)
    left_back, right_back = [], []
    for flip in range(CORES):
        at = slice(flip * RING, (flip + 1) * RING)
        left = [send(rows, r, 0, flip) for r, rows in zip(ring, left_rows[at])]
        right = [send(rows, 0, r, flip) for r, rows in zip(ring, right_rows[at])]
        left, right = expert_mlp(left, right, gate_mat, up_mat, down_mat, 2 * capacity)
        left_back += [send(rows, -r, 0, flip) for r, rows in zip(ring, left)]
        right_back += [send(rows, 0, -r, flip) for r, rows in zip(ring, right)]
    left_own, left_other = combine_rows(left_back, left_place, left_weight, capacity)
    right_own, right_other = combine_rows(right_back, right_place, right_weight, capacity)

    def gathered(left, right):
        sides = [
            sum(send(part, 0, -r).astype(jnp.float32) for r, part in zip(ring, left)),
            sum(send(part, -r, 0).astype(jnp.float32) for r, part in zip(ring, right)),
        ]
        return sides

    other_sides = gathered(left_other, right_other)
    swapped = [lax.ppermute(side.astype(jnp.bfloat16), "half", swap) for side in other_sides]
    own_sides = gathered(left_own, right_own)
    return jnp.concatenate(
        [(a + b.astype(jnp.float32)).astype(jnp.bfloat16) for a, b in zip(own_sides, swapped)], axis=1
    )


def shards(tokens, routes, gate_weights, w_gate, w_up, w_down, saved_inputs, saved_cotangent):
    width = tokens.shape[1]
    gate_mat, up_mat, down_mat = (w_gate[0], w_up[0], w_down[0])
    combined = forward(tokens, routes, gate_weights, gate_mat, up_mat, down_mat)
    replicas = lax.axis_size("edp")
    ring = [(r, (r + 1) % replicas) for r in range(replicas)]
    own_index = lax.axis_index("edp")
    half_width = width // replicas
    half_hidden = gate_mat.shape[1] // replicas
    grad_g = jnp.zeros((half_width, gate_mat.shape[1]), jnp.float32)
    grad_u = jnp.zeros((half_width, gate_mat.shape[1]), jnp.float32)
    grad_d = jnp.zeros((half_hidden, width), jnp.float32)
    inputs, cotangent = saved_inputs[0], saved_cotangent[0]
    for replica in range(replicas):
        hidden, d_gate, d_up = expert_grads(inputs, cotangent, gate_mat, up_mat, down_mat)
        in_cols = lax.dynamic_slice_in_dim(inputs, own_index * half_width, half_width, 1)
        hidden_cols = lax.dynamic_slice_in_dim(hidden, own_index * half_hidden, half_hidden, 1)
        grad_g = grad_g + rounded(
            jnp.einsum("rd,rf->df", in_cols, d_gate, preferred_element_type=jnp.float32)
        )
        grad_u = grad_u + rounded(
            jnp.einsum("rd,rf->df", in_cols, d_up, preferred_element_type=jnp.float32)
        )
        grad_d = grad_d + rounded(
            jnp.einsum("rf,rd->fd", hidden_cols, cotangent, preferred_element_type=jnp.float32)
        )
        if replica + 1 < replicas:
            inputs = lax.ppermute(inputs, "edp", ring)
            cotangent = lax.ppermute(cotangent, "edp", ring)
    grad_gate, grad_up, grad_down = (grad_g[None], grad_u[None], grad_d[None])
    return (combined, grad_gate, grad_up, grad_down)


def solution(mesh):
    replicas = mesh.devices.shape[0]
    split = Mesh(
        mesh.devices.reshape(replicas, HALVES, RING, RING, CORES), ("edp", "half", "z", "x", "core")
    )
    own = ("half", "z", "x", "core")
    tok, rep = P(("edp",) + own, None), P(own, "edp", None)
    return jax.shard_map(
        shards,
        mesh=split,
        in_specs=(tok, tok, tok, P(own), P(own), P(own), rep, rep),
        out_specs=(tok, rep, rep, rep),
        check_vma=False,
    )
```
